1024 devices in a mesh: dp: 16 (over y, z_lo), expert: 16 (over x, core), etp: 4 (over z_hi).
Axes of the slice: x: 8, y: 8, z: 8 (z_hi: 4, z_lo: 2; z = z_hi * 2 + z_lo), core: 2. Of those that a mesh axis runs over, the one named last changes fastest.
Arguments:
- tokens: bfloat16 [16384, 4096], P(('dp', 'expert')), parts along dimension 0, may hold values from -6 to 6
- expert_ids: int32 [16384, 2], P(('dp', 'expert')), parts along dimension 0, may hold values from 0 to 15, all different within a row; in each aligned block of 64 rows (0 to 63, 64 to 127, ...) at most 16 rows name the same one
- route_weights: bfloat16 [16384, 2], P(('dp', 'expert')), parts along dimension 0, may hold values from 0.049804688 to 1
- w_gate: bfloat16 [16, 4096, 1536], P('expert', None, 'etp'), may hold values from -0.09375 to 0.09375
- w_up: bfloat16 [16, 4096, 1536], P('expert', None, 'etp'), may hold values from -0.09375 to 0.09375
- w_down: bfloat16 [16, 1536, 4096], P('expert', 'etp'), may hold values from -0.15625 to 0.15625
Outputs:
- moe_out: bfloat16 [16384, 4096], P(('dp', 'expert'), 'etp'), parts along dimension 0
The draws below stay inside these ranges and needn't reach their ends.
There are 16 independent parts, one for each index of `dp`. The reference program is written for one: setup_inputs(seed, part) draws one part's arguments, and reference() takes and returns one part's arrays. A program takes and returns all parts, laid end to end along the dimension named above; an argument that names none is the same for every part. Nothing has to cross between parts.
Inputs may be any that keep to these rules, and one draw needn't show every extreme that they name: `expert_ids`: within the 64 rows of one index of expert (aligned blocks), a row names 2 different experts and no expert is named by more than 16 rows; some expert is named by exactly 16 rows of some block.
All inputs are finite; a program needn't handle non-finite values.
Results may differ from the reference program's by a relative error of at most 0.01.
Values may be sent and summed in bfloat16 or wider, within the bound.
No kernel may reach another device: no remote copies, remote signals or barrier semaphores. Data moves between devices by JAX's collectives and lax.ppermute only.
A program may use at most 32 MiB of HBM per device.

```python
import math
import jax
import jax.numpy as jnp
import numpy as np
from jax import lax

D = 4096
HIDDEN_SIZE = 1536
TOPK = 2
TOK_DEV = 64
EXPERTS = 16
TOKENS = 1024
CAP = 16
N_EXPERT = 16
N_ETP = 4


def steps_of(own_key, dims, split, low, high):
    gain, own = 1.0, jax.random.fold_in(own_key, 6)
    for position, blocks in split:
        steps = jnp.exp(jax.random.uniform(jax.random.fold_in(own, position), (blocks,), jnp.float32, low / len(split), high / len(split)))
        gain = gain * jnp.repeat(steps, dims[position] // blocks).reshape([-1 if axis == position else 1 for axis in range(len(dims))])
    return gain


def routed_block(rng, own, number, rows, count, top, reach, skew):
    ranking = jax.random.permutation(rng, count)
    packed, ordinary = shares(count, rows * top, reach, skew, True), shares(count, rows * top, reach, skew, False)
    places = jnp.arange(count)

    def named(sizes, turn):
        used = int((sizes > 0).sum())
        fixed = max(1, used // 4)
        shifted = fixed + (places - fixed + turn * (used - fixed)) % max(1, count - fixed)
        return jnp.zeros((count,), jnp.int32).at[ranking[jnp.where(places < fixed, places, shifted)]].set(jnp.asarray(sizes, jnp.int32))

    sizes = jnp.where(number % 4 == 0, named(packed, number // 4), named(ordinary, number - number // 4 - 1))
    mixed = jax.random.permutation(jax.random.fold_in(own, 3), count)
    giver, sink = mixed[0:count // 2 * 2:2], mixed[1:count // 2 * 2:2]
    room = jnp.minimum(sizes[giver] - 1, reach - sizes[sink]) // 2
    room = jnp.where((giver == ranking[0]) | (sink == ranking[0]) | (sizes[sink] == 0), 0, jnp.maximum(room, 0))
    shifted = jax.random.randint(jax.random.fold_in(own, 4), (count // 2,), 0, 1 << 20) % (room + 1)
    sizes = sizes.at[giver].add(-shifted).at[sink].add(shifted)
    labels = jnp.searchsorted(jnp.cumsum(sizes), jnp.arange(rows * top), side="right").astype(jnp.int32)
    listing = labels.reshape(top, rows).T
    listing = listing[jax.random.permutation(jax.random.fold_in(own, 1), rows)]
    turn = jax.random.randint(jax.random.fold_in(own, 2), (rows, 1), 0, top)
    return jnp.take_along_axis(listing, (jnp.arange(top)[None, :] + turn) % top, axis=1)


def shares(number_of, total, reach, slope, full):
    loads = [(1 << 20) // math.isqrt(rank ** slope) + 1 for rank in range(1, number_of + 1)]
    largest = reach if full else min(reach, max(-(-total // number_of), total * loads[0] // sum(loads)))
    least = 1 if total - largest >= number_of - 1 else 0
    counts, rest = [largest] + [least] * (number_of - 1), total - largest - least * (number_of - 1)
    while rest > 0:
        free = [i for i in range(1, number_of) if counts[i] < largest] or [i for i in range(1, number_of) if counts[i] < reach]
        pool, left = sum([loads[i] for i in free]), rest
        for i in free:
            extra = min(reach - counts[i], max(1, left * loads[i] // pool), rest)
            counts[i] = counts[i] + extra
            rest = rest - extra
    return np.array(counts)


def noise(rng, extent, scale, limit, cuts=(), held_as=jnp.bfloat16):
    result = jax.random.normal(rng, extent, jnp.float32) * scale
    if len(cuts) > 0:
        result = steps_of(rng, extent, cuts, -0.22, 0.18) * result
    return jnp.clip(result, min=-limit, max=limit).astype(held_as)


def setup_inputs(seed: int = 0, part: int = 0) -> dict:
    keys = jax.random.split(jax.random.key(seed), 7)
    part_splits = jax.random.split(jax.random.fold_in(keys[6], part), 7)
    tokens = noise(part_splits[0], (TOKENS, D), 1.0, 6.0, ((0, 16),))
    expert_ids_keys = jax.random.split(jax.random.fold_in(part_splits[1], 1), TOKENS // TOK_DEV)
    expert_ids_turns = jax.random.permutation(jax.random.fold_in(part_splits[1], 3), TOKENS // TOK_DEV)
    expert_ids = jax.vmap(lambda own, number: routed_block(jax.random.fold_in(part_splits[1], 2), own, number, TOK_DEV, EXPERTS, TOPK, CAP, 2))(expert_ids_keys, expert_ids_turns).reshape((TOKENS, TOPK))
    route_weights = jnp.clip(jnp.exp(math.log(1.0) - 2.9996462 * jax.random.uniform(part_splits[2], (TOKENS, TOPK), jnp.float32) ** steps_of(part_splits[2], (TOKENS, TOPK), ((0, 16),), -0.2, 0.2)), 0.049804688, 1.0).astype(jnp.bfloat16)
    w_gate = noise(keys[3], (EXPERTS, D, HIDDEN_SIZE), D ** -0.5, 0.09375, ((0, 16), (2, 4)))
    w_up = noise(keys[4], (EXPERTS, D, HIDDEN_SIZE), D ** -0.5, 0.09375, ((0, 16), (2, 4)))
    w_down = noise(keys[5], (EXPERTS, HIDDEN_SIZE, D), HIDDEN_SIZE ** -0.5, 0.15625, ((0, 16), (1, 4)))
    return {"tokens": tokens, "expert_ids": expert_ids, "route_weights": route_weights, "w_gate": w_gate, "w_up": w_up, "w_down": w_down}


def find_slots(expert_ids):
    blocks = expert_ids.reshape(N_EXPERT, TOK_DEV * TOPK)
    onehot = (blocks[:, :, None] == jnp.arange(EXPERTS, dtype=jnp.int32)[None, None, :]).astype(jnp.int32)
    before = jnp.cumsum(onehot, axis=1) - onehot
    slots = jnp.sum(before * onehot, axis=2)
    return slots.reshape(TOKENS, TOPK).astype(jnp.int32)


def reference(tokens, expert_ids, route_weights, w_gate, w_up, w_down):
    slots = find_slots(expert_ids)
    block_of = (jnp.arange(TOKENS, dtype=jnp.int32) // TOK_DEV)[:, None] * jnp.ones((1, TOPK), jnp.int32)
    rows = jnp.broadcast_to(tokens[:, None, :], (TOKENS, TOPK, D))
    buffer = jnp.zeros((EXPERTS, N_EXPERT, CAP, D), jnp.bfloat16)
    buffer = buffer.at[expert_ids, block_of, slots].set(rows)
    group = HIDDEN_SIZE // N_ETP

    def one_expert(index):
        inputs = buffer[index].reshape(N_EXPERT * CAP, D)
        gate = jnp.dot(inputs, w_gate[index], preferred_element_type=jnp.float32)
        up = jnp.dot(inputs, w_up[index], preferred_element_type=jnp.float32)
        hidden = (jax.nn.silu(gate) * up).astype(jnp.bfloat16)
        total = jnp.zeros((N_EXPERT * CAP, D), jnp.float32)
        for part in range(N_ETP):
            piece = jnp.dot(hidden[:, part * group:(part + 1) * group], w_down[index, part * group:(part + 1) * group, :], preferred_element_type=jnp.float32)
            total = total + piece.astype(jnp.bfloat16).astype(jnp.float32)
        return total.astype(jnp.bfloat16).reshape(N_EXPERT, CAP, D)

    expert_out = lax.map(one_expert, jnp.arange(EXPERTS, dtype=jnp.int32))
    picked = expert_out[expert_ids, block_of, slots].astype(jnp.float32)
    weighted = jnp.sum(picked * route_weights.astype(jnp.float32)[:, :, None], axis=1)
    return weighted.astype(jnp.bfloat16)
```

```python
import jax
import jax.numpy as jnp
from jax import lax
from jax.experimental import pallas as pl
from jax.experimental.pallas import tpu as pltpu
from jax.sharding import PartitionSpec as P

def ffn_kernel(x_ref, gate_ref, up_ref, down_ref, out_ref, down_buf, sems):
    sources, quarters, capacity, part = out_ref.shape
    copies = [
        pltpu.make_async_copy(
            down_ref.at[:, pl.ds(q * part, part)], down_buf.at[:, pl.ds(q * part, part)], sems.at[q]
        )
        for q in range(quarters)
    ]
    for copy in copies:
        copy.start()
    x = x_ref[...]
    gate = jnp.dot(x, gate_ref[...], preferred_element_type=jnp.float32)
    up = jnp.dot(x, up_ref[...], preferred_element_type=jnp.float32)
    hidden = (gate / (1.0 + jnp.exp(-gate)) * up).astype(jnp.bfloat16)
    for q in range(quarters):
        copies[q].wait()
        out = jnp.dot(hidden, down_buf[:, pl.ds(q * part, part)], preferred_element_type=jnp.float32)
        out_ref[:, q] = out.astype(out_ref.dtype).reshape(sources, capacity, part)


def ffn(arrived, w_gate, w_up, w_down, sources, quarters):
    rows, width = arrived.shape
    hidden_units = w_gate.shape[1]
    in_vmem = pl.BlockSpec(memory_space=pltpu.VMEM)
    return pl.pallas_call(
        ffn_kernel,
        out_shape=jax.ShapeDtypeStruct(
            (sources, quarters, rows // sources, width // quarters), jnp.bfloat16
        ),
        in_specs=[in_vmem, in_vmem, in_vmem, pl.BlockSpec(memory_space=pltpu.HBM)],
        out_specs=in_vmem,
        scratch_shapes=[
            pltpu.VMEM((hidden_units, width), jnp.bfloat16),
            pltpu.SemaphoreType.DMA((quarters,)),
        ],
        compiler_params=pltpu.CompilerParams(vmem_limit_bytes=32 * 2**20),
        cost_estimate=pl.CostEstimate(
            flops=6 * rows * width * hidden_units,
            bytes_accessed=2 * (2 * rows * width + 3 * width * hidden_units),
            transcendentals=rows * hidden_units,
        ),
    )(arrived, w_gate, w_up, w_down)


def per_device(tokens, expert_ids, route_weights, w_gate, w_up, w_down):
    tok_rows, width = tokens.shape
    route_count = expert_ids.shape[1]
    sources = lax.axis_size("expert")
    quarters = lax.axis_size("etp")
    experts = sources
    capacity = 2 * tok_rows * route_count // experts
    quarter = width // quarters
    flat_ids = expert_ids.reshape(-1)
    onehot = (flat_ids[:, None] == jnp.arange(experts, dtype=jnp.int32)[None, :]).astype(jnp.int32)
    before = jnp.cumsum(onehot, axis=0) - onehot
    slots = jnp.sum(before * onehot, axis=1)
    position = (flat_ids * capacity + slots).reshape(tok_rows, route_count)
    targets = jnp.arange(experts * capacity, dtype=jnp.int32)
    hits = position[:, :, None] == targets[None, None, :]
    dispatch_map = jnp.transpose(jnp.any(hits, axis=1)).astype(jnp.bfloat16)
    outgoing = jnp.dot(dispatch_map, tokens, preferred_element_type=jnp.float32).astype(
        jnp.bfloat16
    )
    arrived = lax.all_to_all(
        outgoing.reshape(experts, capacity, width),
        "expert",
        split_axis=0,
        concat_axis=0,
        tiled=True,
    )
    partial_out = ffn(
        arrived.reshape(sources * capacity, width), w_gate[0], w_up[0], w_down[0], sources, quarters
    )
    returned = lax.all_to_all(
        partial_out.reshape(sources * quarters, capacity, quarter),
        ("expert", "etp"),
        split_axis=0,
        concat_axis=0,
        tiled=True,
    )
    row = jnp.arange(experts * quarters * capacity, dtype=jnp.int32)
    place = row // (quarters * capacity) * capacity + row % capacity
    spread = position[:, :, None] == place[None, None, :]
    combine_map = jnp.sum(
        jnp.where(spread, route_weights[:, :, None], jnp.zeros((), jnp.bfloat16)), axis=1
    )
    mixed = jnp.dot(
        combine_map,
        returned.reshape(experts * quarters * capacity, quarter),
        preferred_element_type=jnp.float32,
    )
    return mixed.astype(jnp.bfloat16)


def solution(mesh):
    return jax.shard_map(
        per_device,
        mesh=mesh,
        in_specs=(
            P(("dp", "expert"), None),
            P(("dp", "expert"), None),
            P(("dp", "expert"), None),
            P("expert", None, "etp"),
            P("expert", None, "etp"),
            P("expert", "etp", None),
        ),
        out_specs=P(("dp", "expert"), "etp"),
        check_vma=False,
    )
```

```python
import jax
import jax.numpy as jnp
from jax import lax
from jax.experimental import pallas as pl
from jax.experimental.pallas import tpu as pltpu
from jax.sharding import PartitionSpec as P


DP_STEP = 2


def shift(x, axis, by):
    count = lax.axis_size(axis)
    return lax.ppermute(x, axis, [(i, (i + by) % count) for i in range(count)])


STEPS = 4


def hidden_kernel(x_ref, gate_ref, up_ref, out_ref, x_buf, gate_buf, up_buf, sems):
    rows, width = x_ref.shape
    depth = width // STEPS
    copies = []
    for k in range(STEPS):
        part = pl.ds(k * depth, depth)
        copies.append(
            (
                pltpu.make_async_copy(x_ref.at[:, part], x_buf.at[:, part], sems.at[0, k]),
                pltpu.make_async_copy(gate_ref.at[part], gate_buf.at[part], sems.at[1, k]),
                pltpu.make_async_copy(up_ref.at[part], up_buf.at[part], sems.at[2, k]),
            )
        )
    for group in copies:
        for copy in group:
            copy.start()
    gate = jnp.zeros((rows, gate_ref.shape[1]), jnp.float32)
    up = jnp.zeros((rows, gate_ref.shape[1]), jnp.float32)
    for k in range(STEPS):
        for copy in copies[k]:
            copy.wait()
        part = pl.ds(k * depth, depth)
        x = x_buf[:, part]
        gate += jnp.dot(x, gate_buf[part, :], preferred_element_type=jnp.float32)
        up += jnp.dot(x, up_buf[part, :], preferred_element_type=jnp.float32)
    out_ref[...] = (gate / (1.0 + jnp.exp(-gate)) * up).astype(out_ref.dtype)


def hidden_units(arrived, w_gate, w_up):
    rows, width = arrived.shape
    units = w_gate.shape[1]
    in_vmem = pl.BlockSpec(memory_space=pltpu.VMEM)
    in_hbm = pl.BlockSpec(memory_space=pltpu.HBM)
    return pl.pallas_call(
        hidden_kernel,
        out_shape=jax.ShapeDtypeStruct((rows, units), jnp.bfloat16),
        in_specs=[in_hbm, in_hbm, in_hbm],
        out_specs=in_vmem,
        scratch_shapes=[
            pltpu.VMEM((rows, width), jnp.bfloat16),
            pltpu.VMEM((width, units), jnp.bfloat16),
            pltpu.VMEM((width, units), jnp.bfloat16),
            pltpu.SemaphoreType.DMA((3, STEPS)),
        ],
        compiler_params=pltpu.CompilerParams(vmem_limit_bytes=56 * 2**20),
        cost_estimate=pl.CostEstimate(
            flops=4 * rows * width * units,
            bytes_accessed=2 * (rows * width + 2 * width * units + rows * units),
            transcendentals=rows * units,
        ),
    )(arrived, w_gate, w_up)


def down_kernel(*refs):
    out_ref = refs[-1]
    groups = (len(refs) - 4) // 2
    hidden, own, fetched = refs[: groups + 1], refs[groups + 1], refs[groups + 2 : -3]
    others = refs[-3:-1]
    units = own.shape[0]
    half, piece = fetched[0].shape[1], others[0].shape[1]
    odd = lax.rem(lax.div(lax.axis_index("dp"), DP_STEP), 2)

    def project(start, columns, blocks):
        start = pl.multiple_of(start, piece)
        total = jnp.dot(hidden[0][...], own[:, pl.ds(start, columns)], preferred_element_type=jnp.float32)
        for k in range(groups):
            total += jnp.dot(hidden[k + 1][...], blocks(k), preferred_element_type=jnp.float32)
        out_ref[:, pl.ds(start, columns)] = total.astype(out_ref.dtype)

    project(odd * half, half, lambda k: fetched[k][...])
    for side in range(2):
        project(
            (1 - odd) * half + side * piece,
            piece,
            lambda k: others[side][pl.ds(k * units, units), :],
        )


def project_down(hidden, own, fetched, others):
    rows, units = hidden[0].shape
    quarter = own.shape[1]
    in_vmem = pl.BlockSpec(memory_space=pltpu.VMEM)
    operands = (*hidden, own, *fetched, *others)
    return pl.pallas_call(
        down_kernel,
        out_shape=jax.ShapeDtypeStruct((rows, quarter), jnp.bfloat16),
        in_specs=[in_vmem] * len(operands),
        out_specs=in_vmem,
        compiler_params=pltpu.CompilerParams(vmem_limit_bytes=24 * 2**20),
        cost_estimate=pl.CostEstimate(
            flops=2 * len(hidden) * rows * units * quarter,
            bytes_accessed=2 * len(hidden) * (rows * units + units * quarter) + 2 * rows * quarter,
            transcendentals=0,
        ),
    )(*operands)


def down_weights(w_down, quarter, quarters):
    here = lax.axis_index("etp")
    odd = (lax.axis_index("dp") // DP_STEP) % 2
    half, units = quarter // 2, w_down.shape[0]
    own = lax.dynamic_slice(w_down, (0, here * quarter), (units, quarter))
    parts = [
        lax.dynamic_slice(w_down, (0, (here + k) % quarters * quarter + odd * half), (units, half))
        for k in range(1, quarters)
    ]
    fetched = [shift(part, "etp", k) for k, part in enumerate(parts, 1)]
    stacked = jnp.concatenate(fetched, axis=0)
    others = (
        shift(stacked[:, : half // 2], "dp", DP_STEP),
        shift(stacked[:, half // 2 :], "dp", -DP_STEP),
    )
    return own, fetched, others


def per_device(tokens, expert_ids, route_weights, w_gate, w_up, w_down):
    tok_rows, width = tokens.shape
    route_count = expert_ids.shape[1]
    sources = lax.axis_size("expert")
    quarters = lax.axis_size("etp")
    experts = sources
    capacity = 2 * tok_rows * route_count // experts
    quarter = width // quarters
    flat_ids = expert_ids.reshape(-1)
    onehot = (flat_ids[:, None] == jnp.arange(experts, dtype=jnp.int32)[None, :]).astype(jnp.int32)
    before = jnp.cumsum(onehot, axis=0) - onehot
    slots = jnp.sum(before * onehot, axis=1)
    position = (flat_ids * capacity + slots).reshape(tok_rows, route_count)
    targets = jnp.arange(experts * capacity, dtype=jnp.int32)
    hits = position[:, :, None] == targets[None, None, :]
    dispatch_map = jnp.transpose(jnp.any(hits, axis=1)).astype(jnp.bfloat16)
    combine_map = jnp.sum(
        jnp.where(hits, route_weights[:, :, None], jnp.zeros((), jnp.bfloat16)), axis=1
    )
    outgoing = jnp.dot(dispatch_map, tokens, preferred_element_type=jnp.float32).astype(
        jnp.bfloat16
    )
    arrived = lax.all_to_all(
        outgoing.reshape(experts, capacity, width), "expert", split_axis=0, concat_axis=0, tiled=True
    )
    own, fetched, others = down_weights(w_down[0], quarter, quarters)
    hidden = hidden_units(arrived.reshape(sources * capacity, width), w_gate[0], w_up[0])
    gathered = [hidden] + [shift(hidden, "etp", k) for k in range(1, quarters)]
    expert_out = project_down(gathered, own, fetched, others)
    returned = lax.all_to_all(
        expert_out.reshape(sources, capacity, quarter), "expert", split_axis=0, concat_axis=0, tiled=True
    )
    mixed = jnp.dot(
        combine_map,
        returned.reshape(experts * capacity, quarter),
        preferred_element_type=jnp.float32,
    )
    return mixed.astype(jnp.bfloat16)


def solution(mesh):
    return jax.shard_map(
        per_device,
        mesh=mesh,
        in_specs=(
            P(("dp", "expert"), None),
            P(("dp", "expert"), None),
            P(("dp", "expert"), None),
            P("expert", None, "etp"),
            P("expert", None, "etp"),
            P("expert", "etp", None),
        ),
        out_specs=P(("dp", "expert"), "etp"),
        check_vma=False,
    )
```

```python
import jax
import jax.numpy as jnp
from jax import lax
from jax.experimental import pallas as pl
from jax.experimental.pallas import tpu as pltpu
from jax.sharding import PartitionSpec as P


STEPS = 4
BF16, F32 = jnp.bfloat16, jnp.float32
IN_VMEM = pl.BlockSpec(memory_space=pltpu.VMEM)
IN_HBM = pl.BlockSpec(memory_space=pltpu.HBM)


def shift(x, axis, by):
    count = lax.axis_size(axis)
    return lax.ppermute(x, axis, [(i, (i + by) % count) for i in range(count)])


def dispatch_kernel(ids_ref, weights_ref, tokens_ref, out_ref, combine_ref, chosen):
    experts, capacity = combine_ref.shape[0], combine_ref.shape[1]
    routes, rows = ids_ref.shape

    @pl.when(pl.program_id(0) == 0)
    def _():
        expert = lax.broadcasted_iota(jnp.int32, (experts, rows), 0)
        named = jnp.zeros((experts, rows), F32)
        weight = jnp.zeros((experts, rows), F32)
        for k in range(routes):
            hit = ids_ref[k : k + 1, :] == expert
            named = jnp.where(hit, 1.0, named)
            weight = jnp.where(hit, weights_ref[k : k + 1, :].astype(F32), weight)
        earlier = lax.broadcasted_iota(jnp.int32, (rows, rows), 0) < lax.broadcasted_iota(
            jnp.int32, (rows, rows), 1
        )
        slot = jnp.dot(
            named.astype(BF16), jnp.where(earlier, 1.0, 0.0).astype(BF16), preferred_element_type=F32
        ).astype(jnp.int32)
        slot = jnp.where(named > 0.0, slot, -1)
        place = lax.broadcasted_iota(jnp.int32, (experts, capacity, rows), 1)
        taken = slot[:, None, :] == place
        chosen[...] = jnp.where(taken, 1.0, 0.0).reshape(experts * capacity, rows).astype(BF16)
        combine_ref[...] = jnp.where(taken, weight[:, None, :], 0.0).astype(BF16)

    out_ref[...] = jnp.dot(chosen[...], tokens_ref[...], preferred_element_type=F32).astype(BF16)


def dispatch_rows(expert_ids, route_weights, tokens, experts, capacity):
    rows, width = tokens.shape
    routes = expert_ids.shape[1]
    small = pl.BlockSpec((routes, rows), lambda i: (0, 0))
    return pl.pallas_call(
        dispatch_kernel,
        grid=(STEPS,),
        out_shape=(
            jax.ShapeDtypeStruct((experts * capacity, width), BF16),
            jax.ShapeDtypeStruct((experts, capacity, rows), BF16),
        ),
        in_specs=[small, small, pl.BlockSpec((rows, width // STEPS), lambda i: (0, i))],
        out_specs=(
            pl.BlockSpec((experts * capacity, width // STEPS), lambda i: (0, i)),
            pl.BlockSpec((experts, capacity, rows), lambda i: (0, 0, 0)),
        ),
        scratch_shapes=[pltpu.VMEM((experts * capacity, rows), BF16)],
        compiler_params=pltpu.CompilerParams(vmem_limit_bytes=60 * 2**20),
        cost_estimate=pl.CostEstimate(
            flops=2 * experts * capacity * rows * width,
            bytes_accessed=2 * (experts * capacity + rows) * width,
            transcendentals=0,
        ),
    )(expert_ids.T, route_weights.T, tokens)


def hidden_kernel(x_ref, gate_ref, up_ref, out_ref, x_buf, weights, sems):
    rows, width = x_ref.shape
    units = gate_ref.shape[1]
    depth = width // STEPS
    copies = []
    for k in range(STEPS):
        part = pl.ds(k * depth, depth)
        copies.append(
            (
                pltpu.make_async_copy(x_ref.at[:, part], x_buf.at[:, part], sems.at[0, k]),
                pltpu.make_async_copy(
                    gate_ref.at[part], weights.at[part, pl.ds(0, units)], sems.at[1, k]
                ),
                pltpu.make_async_copy(
                    up_ref.at[part], weights.at[part, pl.ds(units, units)], sems.at[2, k]
                ),
            )
        )
    for group in copies:
        for copy in group:
            copy.start()
    total = jnp.zeros((rows, 2 * units), F32)
    for k in range(STEPS):
        for copy in copies[k]:
            copy.wait()
        part = pl.ds(k * depth, depth)
        total += jnp.dot(x_buf[:, part], weights[part, :], preferred_element_type=F32)
    gate, up = total[:, :units], total[:, units:]
    out_ref[...] = (gate / (1.0 + jnp.exp(-gate)) * up).astype(out_ref.dtype)


def hidden_units(arrived, w_gate, w_up):
    rows, width = arrived.shape
    units = w_gate.shape[1]
    return pl.pallas_call(
        hidden_kernel,
        out_shape=jax.ShapeDtypeStruct((rows, units), BF16),
        in_specs=[IN_HBM] * 3,
        out_specs=IN_VMEM,
        scratch_shapes=[
            pltpu.VMEM((rows, width), BF16),
            pltpu.VMEM((width, 2 * units), BF16),
            pltpu.SemaphoreType.DMA((3, STEPS)),
        ],
        compiler_params=pltpu.CompilerParams(vmem_limit_bytes=56 * 2**20),
        cost_estimate=pl.CostEstimate(
            flops=4 * rows * width * units,
            bytes_accessed=2 * (rows * width + 2 * width * units + rows * units),
            transcendentals=rows * units,
        ),
    )(arrived, w_gate, w_up)


def down_kernel(mine, after, before, own_low, own_high, sent_low, sent_high, out_ref):
    sources, quarters, capacity, part = out_ref.shape
    pairs = ((after, own_low, sent_low), (before, own_high, sent_high))
    for side, (other, own, sent) in enumerate(pairs):
        for j in range(quarters // 2):
            cols = pl.ds(j * part, part)
            total = jnp.dot(mine[...], own[:, cols], preferred_element_type=F32)
            total += jnp.dot(other[...], sent[:, cols], preferred_element_type=F32)
            out_ref[:, side * (quarters // 2) + j] = total.astype(BF16).reshape(
                sources, capacity, part
            )


def project_down(operands, sources, quarters, capacity):
    rows, units = operands[0].shape
    width = operands[-1].shape[1]
    return pl.pallas_call(
        down_kernel,
        out_shape=jax.ShapeDtypeStruct((sources, quarters, capacity, 2 * width // quarters), BF16),
        in_specs=[IN_VMEM] * len(operands),
        out_specs=IN_VMEM,
        compiler_params=pltpu.CompilerParams(vmem_limit_bytes=24 * 2**20),
        cost_estimate=pl.CostEstimate(
            flops=8 * rows * units * width,
            bytes_accessed=2 * (3 * rows * units + 4 * units * width + 2 * rows * width),
            transcendentals=0,
        ),
    )(*operands)


def combine_kernel(maps_ref, rows_ref, out_ref):
    rows = maps_ref.shape[0] // 2
    half = rows_ref.shape[1]
    total = jnp.dot(maps_ref[...], rows_ref[...], preferred_element_type=F32).astype(BF16)
    out_ref[:, :half] = total[:rows]
    out_ref[:, half:] = total[rows:]


def combine_rows(maps, returned):
    rows, depth = maps.shape
    half = returned.shape[1]
    return pl.pallas_call(
        combine_kernel,
        out_shape=jax.ShapeDtypeStruct((rows // 2, 2 * half), BF16),
        in_specs=[IN_VMEM] * 2,
        out_specs=IN_VMEM,
        compiler_params=pltpu.CompilerParams(vmem_limit_bytes=24 * 2**20),
        cost_estimate=pl.CostEstimate(
            flops=2 * rows * depth * half,
            bytes_accessed=2 * (rows * depth + depth * half + rows * half),
            transcendentals=0,
        ),
    )(maps, returned)


def weight_columns(w_down, first, half, choice):
    units = w_down.shape[0]
    start = first + choice * half
    return jnp.concatenate(
        [lax.dynamic_slice(w_down, (0, start + k * 2 * half), (units, half)) for k in range(2)], axis=1
    )


def per_device(tokens, expert_ids, route_weights, w_gate, w_up, w_down):
    tok_rows, width = tokens.shape
    route_count = expert_ids.shape[1]
    sources = lax.axis_size("expert")
    quarters = lax.axis_size("etp")
    experts = sources
    capacity = 2 * tok_rows * route_count // experts
    quarter = width // quarters
    half = quarter // 2
    here = lax.axis_index("etp")
    odd = here % 2

    outgoing, combine = dispatch_rows(expert_ids, route_weights, tokens, experts, capacity)
    arrived = lax.all_to_all(
        outgoing.reshape(experts, capacity, width), "expert", split_axis=0, concat_axis=0, tiled=True
    )

    down = w_down[0]
    own_low = weight_columns(down, 0, half, odd)
    own_high = weight_columns(down, width // 2, half, 1 - odd)
    sent_low = shift(weight_columns(down, 0, half, 1 - odd), "etp", -1)
    sent_high = shift(weight_columns(down, width // 2, half, odd), "etp", 1)

    mine = hidden_units(arrived.reshape(sources * capacity, width), w_gate[0], w_up[0])
    after, before = shift(mine, "etp", -1), shift(mine, "etp", 1)
    expert_out = project_down(
        (mine, after, before, own_low, own_high, sent_low, sent_high), sources, quarters, capacity
    )
    returned = lax.all_to_all(
        expert_out.reshape(sources * quarters, capacity, half),
        ("expert", "etp"),
        split_axis=0,
        concat_axis=0,
        tiled=True,
    )
    first_half = (jnp.arange(quarters) % 2 == here // (quarters // 2))[None, None, :, None]
    weights = jnp.transpose(combine.reshape(experts * capacity, tok_rows))
    spread = jnp.broadcast_to(
        weights.reshape(tok_rows, experts, 1, capacity), (tok_rows, experts, quarters, capacity)
    )
    maps = jnp.stack([jnp.where(first_half, spread, 0), jnp.where(first_half, 0, spread)])
    return combine_rows(
        maps.reshape(2 * tok_rows, experts * quarters * capacity),
        returned.reshape(experts * quarters * capacity, half),
    )


def solution(mesh):
    return jax.shard_map(
        per_device,
        mesh=mesh,
        in_specs=(
            P(("dp", "expert"), None),
            P(("dp", "expert"), None),
            P(("dp", "expert"), None),
            P("expert", None, "etp"),
            P("expert", None, "etp"),
            P("expert", "etp", None),
        ),
        out_specs=P(("dp", "expert"), "etp"),
        check_vma=False,
    )
```

```python
import jax
import jax.numpy as jnp
from jax import lax
from jax.experimental import pallas as pl
from jax.experimental.pallas import tpu as pltpu
from jax.sharding import PartitionSpec as P


STEPS = 2
PIECES = 4
DP_STEP = 2
SHARERS = 4
BF16, F32 = jnp.bfloat16, jnp.float32
IN_VMEM = pl.BlockSpec(memory_space=pltpu.VMEM)
IN_HBM = pl.BlockSpec(memory_space=pltpu.HBM)


def shift(x, axis, by):
    count = lax.axis_size(axis)
    return lax.ppermute(x, axis, [(i, (i + by) % count) for i in range(count)])


def dispatch_kernel(ids_ref, weights_ref, tokens_ref, out_ref, combine_ref, chosen):
    experts, capacity = combine_ref.shape[0], combine_ref.shape[1]
    routes, rows = ids_ref.shape

    @pl.when(pl.program_id(0) == 0)
    def _():
        expert = lax.broadcasted_iota(jnp.int32, (experts, rows), 0)
        named = jnp.zeros((experts, rows), F32)
        weight = jnp.zeros((experts, rows), F32)
        for k in range(routes):
            hit = ids_ref[k : k + 1, :] == expert
            named = jnp.where(hit, 1.0, named)
            weight = jnp.where(hit, weights_ref[k : k + 1, :].astype(F32), weight)
        earlier = lax.broadcasted_iota(jnp.int32, (rows, rows), 0) < lax.broadcasted_iota(
            jnp.int32, (rows, rows), 1
        )
        slot = jnp.dot(
            named.astype(BF16), jnp.where(earlier, 1.0, 0.0).astype(BF16), preferred_element_type=F32
        ).astype(jnp.int32)
        slot = jnp.where(named > 0.0, slot, -1)
        place = lax.broadcasted_iota(jnp.int32, (experts, capacity, rows), 1)
        taken = slot[:, None, :] == place
        chosen[...] = jnp.where(taken, 1.0, 0.0).reshape(experts * capacity, rows).astype(BF16)
        combine_ref[...] = jnp.where(taken, weight[:, None, :], 0.0).astype(BF16)

    out_ref[...] = jnp.dot(chosen[...], tokens_ref[...], preferred_element_type=F32).astype(BF16)


def dispatch_rows(expert_ids, route_weights, tokens, experts, capacity):
    rows, width = tokens.shape
    routes = expert_ids.shape[1]
    small = pl.BlockSpec((routes, rows), lambda i: (0, 0))
    return pl.pallas_call(
        dispatch_kernel,
        grid=(STEPS,),
        out_shape=(
            jax.ShapeDtypeStruct((experts * capacity, width), BF16),
            jax.ShapeDtypeStruct((experts, capacity, rows), BF16),
        ),
        in_specs=[small, small, pl.BlockSpec((rows, width // STEPS), lambda i: (0, i))],
        out_specs=(
            pl.BlockSpec((experts * capacity, width // STEPS), lambda i: (0, i)),
            pl.BlockSpec((experts, capacity, rows), lambda i: (0, 0, 0)),
        ),
        scratch_shapes=[pltpu.VMEM((experts * capacity, rows), BF16)],
        compiler_params=pltpu.CompilerParams(vmem_limit_bytes=60 * 2**20),
        cost_estimate=pl.CostEstimate(
            flops=2 * experts * capacity * rows * width,
            bytes_accessed=2 * (experts * capacity + rows) * width,
            transcendentals=0,
        ),
    )(expert_ids.T, route_weights.T, tokens)


def hidden_kernel(x_ref, gate_ref, up_ref, out_ref, x_buf, weights, sems):
    rows, width = x_ref.shape
    units = gate_ref.shape[1]
    depth = width // PIECES
    copies = []
    for k in range(PIECES):
        part = pl.ds(k * depth, depth)
        copies.append(
            (
                pltpu.make_async_copy(x_ref.at[:, part], x_buf.at[:, part], sems.at[2, k]),
                pltpu.make_async_copy(
                    gate_ref.at[part], weights.at[part, pl.ds(0, units)], sems.at[0, k]
                ),
                pltpu.make_async_copy(
                    up_ref.at[part], weights.at[part, pl.ds(units, units)], sems.at[1, k]
                ),
            )
        )
    for group in copies:
        for copy in group:
            copy.start()
    total = jnp.zeros((rows, 2 * units), F32)
    for k in range(PIECES):
        for copy in copies[k]:
            copy.wait()
        part = pl.ds(k * depth, depth)
        total += jnp.dot(x_buf[:, part], weights[part, :], preferred_element_type=F32)
    gate, up = total[:, :units], total[:, units:]
    out_ref[...] = (gate / (1.0 + jnp.exp(-gate)) * up).astype(out_ref.dtype)


def hidden_units(arrived, w_gate, w_up):
    rows, width = arrived.shape
    units = w_gate.shape[1]
    return pl.pallas_call(
        hidden_kernel,
        out_shape=pltpu.VMEM((rows, units), BF16),
        in_specs=[IN_HBM] * 3,
        out_specs=IN_VMEM,
        scratch_shapes=[
            pltpu.VMEM((rows, width), BF16),
            pltpu.VMEM((width, 2 * units), BF16),
            pltpu.SemaphoreType.DMA((3, PIECES)),
        ],
        compiler_params=pltpu.CompilerParams(vmem_limit_bytes=56 * 2**20),
        cost_estimate=pl.CostEstimate(
            flops=4 * rows * width * units,
            bytes_accessed=2 * (rows * width + 2 * width * units + rows * units),
            transcendentals=rows * units,
        ),
    )(arrived, w_gate, w_up)


def down_kernel(mine, other1, other2, other3, own, fetched, left, right, low, high, out_ref):
    piece, side = fetched.shape[1], low.shape[1]
    here = lax.rem(lax.div(lax.axis_index("dp"), DP_STEP), SHARERS)
    others = jnp.concatenate([other1[...], other2[...], other3[...]], axis=1)

    def project(start, block):
        columns = pl.ds(pl.multiple_of(start, side), block.shape[1])
        total = jnp.dot(mine[...], own[:, columns], preferred_element_type=F32)
        total += jnp.dot(others, block[...], preferred_element_type=F32)
        out_ref[:, columns] = total.astype(out_ref.dtype)

    project(here * piece, fetched)
    project(lax.rem(here + SHARERS - 1, SHARERS) * piece, left)
    project(lax.rem(here + 1, SHARERS) * piece, right)
    far = lax.rem(here + 2, SHARERS) * piece
    project(far, low)
    project(far + side, high)


def project_down(operands):
    rows, units = operands[0].shape
    own = operands[4]
    quarter = own.shape[1]
    return pl.pallas_call(
        down_kernel,
        out_shape=jax.ShapeDtypeStruct((rows, quarter), BF16),
        in_specs=[IN_VMEM] * len(operands),
        out_specs=IN_VMEM,
        compiler_params=pltpu.CompilerParams(vmem_limit_bytes=16 * 2**20),
        cost_estimate=pl.CostEstimate(
            flops=8 * rows * units * quarter,
            bytes_accessed=8 * (rows * units + units * quarter) + 2 * rows * quarter,
            transcendentals=0,
        ),
    )(*operands)


def down_weights(w_down, quarter, quarters):
    here = lax.axis_index("etp")
    units, piece = w_down.shape[0], quarter // SHARERS
    block = (lax.axis_index("dp") // DP_STEP) % SHARERS
    own = lax.dynamic_slice(w_down, (0, here * quarter), (units, quarter))
    parts = [
        lax.dynamic_slice(w_down, (0, (here + k) % quarters * quarter + block * piece), (units, piece))
        for k in range(1, quarters)
    ]
    fetched = jnp.concatenate([shift(part, "etp", k) for k, part in enumerate(parts, 1)], axis=0)
    spread = (
        shift(fetched, "dp", DP_STEP),
        shift(fetched, "dp", -DP_STEP),
        shift(fetched[:, : piece // 2], "dp", 2 * DP_STEP),
        shift(fetched[:, piece // 2 :], "dp", -2 * DP_STEP),
    )
    return own, fetched, *spread


def per_device(tokens, expert_ids, route_weights, w_gate, w_up, w_down):
    tok_rows, width = tokens.shape
    route_count = expert_ids.shape[1]
    sources = lax.axis_size("expert")
    quarters = lax.axis_size("etp")
    experts = sources
    capacity = 2 * tok_rows * route_count // experts
    quarter = width // quarters

    outgoing, combine = dispatch_rows(expert_ids, route_weights, tokens, experts, capacity)
    arrived = lax.all_to_all(
        outgoing.reshape(experts, capacity, width), "expert", split_axis=0, concat_axis=0, tiled=True
    )
    blocks = down_weights(w_down[0], quarter, quarters)
    mine = hidden_units(arrived.reshape(sources * capacity, width), w_gate[0], w_up[0])
    others = [shift(mine, "etp", k) for k in range(1, quarters)]
    expert_out = project_down((mine, *others, *blocks))
    returned = lax.all_to_all(
        expert_out.reshape(sources, capacity, quarter), "expert", split_axis=0, concat_axis=0, tiled=True
    )
    return lax.dot_general(
        combine.reshape(experts * capacity, tok_rows),
        returned.reshape(experts * capacity, quarter),
        (((0,), (0,)), ((), ())),
        preferred_element_type=F32,
    ).astype(BF16)


def solution(mesh):
    return jax.shard_map(
        per_device,
        mesh=mesh,
        in_specs=(
            P(("dp", "expert"), None),
            P(("dp", "expert"), None),
            P(("dp", "expert"), None),
            P("expert", None, "etp"),
            P("expert", None, "etp"),
            P("expert", "etp", None),
        ),
        out_specs=P(("dp", "expert"), "etp"),
        check_vma=False,
    )
```

```python
import jax
import jax.numpy as jnp
from jax import lax
from jax.experimental import pallas as pl
from jax.experimental.pallas import tpu as pltpu
from jax.sharding import PartitionSpec as P


STEPS = 2
PIECES = 4
DP_STEP = 2
SHARERS = 4
BF16, F32 = jnp.bfloat16, jnp.float32
IN_VMEM = pl.BlockSpec(memory_space=pltpu.VMEM)
IN_HBM = pl.BlockSpec(memory_space=pltpu.HBM)


def shift(x, axis, by):
    count = lax.axis_size(axis)
    return lax.ppermute(x, axis, [(i, (i + by) % count) for i in range(count)])


def dispatch_kernel(ids_ref, weights_ref, tokens_ref, out_ref, combine_ref, chosen):
    experts, capacity = combine_ref.shape[0], combine_ref.shape[1]
    routes, rows = ids_ref.shape

    @pl.when(pl.program_id(0) == 0)
    def _():
        expert = lax.broadcasted_iota(jnp.int32, (experts, rows), 0)
        named = jnp.zeros((experts, rows), F32)
        weight = jnp.zeros((experts, rows), F32)
        for k in range(routes):
            hit = ids_ref[k : k + 1, :] == expert
            named = jnp.where(hit, 1.0, named)
            weight = jnp.where(hit, weights_ref[k : k + 1, :].astype(F32), weight)
        earlier = lax.broadcasted_iota(jnp.int32, (rows, rows), 0) < lax.broadcasted_iota(
            jnp.int32, (rows, rows), 1
        )
        slot = jnp.dot(
            named.astype(BF16), jnp.where(earlier, 1.0, 0.0).astype(BF16), preferred_element_type=F32
        ).astype(jnp.int32)
        slot = jnp.where(named > 0.0, slot, -1)
        place = lax.broadcasted_iota(jnp.int32, (experts, capacity, rows), 1)
        taken = slot[:, None, :] == place
        chosen[...] = jnp.where(taken, 1.0, 0.0).reshape(experts * capacity, rows).astype(BF16)
        combine_ref[...] = jnp.where(taken, weight[:, None, :], 0.0).astype(BF16)

    out_ref[...] = jnp.dot(chosen[...], tokens_ref[...], preferred_element_type=F32).astype(BF16)


def dispatch_rows(expert_ids, route_weights, tokens, experts, capacity):
    rows, width = tokens.shape
    routes = expert_ids.shape[1]
    small = pl.BlockSpec((routes, rows), lambda i: (0, 0))
    return pl.pallas_call(
        dispatch_kernel,
        grid=(STEPS,),
        out_shape=(
            jax.ShapeDtypeStruct((experts * capacity, width), BF16),
            jax.ShapeDtypeStruct((experts, capacity, rows), BF16),
        ),
        in_specs=[small, small, pl.BlockSpec((rows, width // STEPS), lambda i: (0, i))],
        out_specs=(
            pl.BlockSpec((experts * capacity, width // STEPS), lambda i: (0, i)),
            pl.BlockSpec((experts, capacity, rows), lambda i: (0, 0, 0)),
        ),
        scratch_shapes=[pltpu.VMEM((experts * capacity, rows), BF16)],
        compiler_params=pltpu.CompilerParams(vmem_limit_bytes=60 * 2**20),
        cost_estimate=pl.CostEstimate(
            flops=2 * experts * capacity * rows * width,
            bytes_accessed=2 * (experts * capacity + rows) * width,
            transcendentals=0,
        ),
    )(expert_ids.T, route_weights.T, tokens)


def hidden_kernel(x_ref, gate_ref, up_ref, out_ref, x_buf, weights, sems):
    rows, width = x_ref.shape
    units = gate_ref.shape[1]
    depth = width // PIECES
    copies = []
    for k in range(PIECES):
        part = pl.ds(k * depth, depth)
        copies.append(
            (
                pltpu.make_async_copy(x_ref.at[:, part], x_buf.at[:, part], sems.at[2, k]),
                pltpu.make_async_copy(
                    gate_ref.at[part], weights.at[part, pl.ds(0, units)], sems.at[0, k]
                ),
                pltpu.make_async_copy(
                    up_ref.at[part], weights.at[part, pl.ds(units, units)], sems.at[1, k]
                ),
            )
        )
    for group in copies:
        for copy in group:
            copy.start()
    total = jnp.zeros((rows, 2 * units), F32)
    for k in range(PIECES):
        for copy in copies[k]:
            copy.wait()
        part = pl.ds(k * depth, depth)
        total += jnp.dot(x_buf[:, part], weights[part, :], preferred_element_type=F32)
    gate, up = total[:, :units], total[:, units:]
    out_ref[...] = (gate / (1.0 + jnp.exp(-gate)) * up).astype(out_ref.dtype)


def hidden_units(arrived, w_gate, w_up):
    rows, width = arrived.shape
    units = w_gate.shape[1]
    return pl.pallas_call(
        hidden_kernel,
        out_shape=pltpu.VMEM((rows, units), BF16),
        in_specs=[IN_HBM] * 3,
        out_specs=IN_VMEM,
        scratch_shapes=[
            pltpu.VMEM((rows, width), BF16),
            pltpu.VMEM((width, 2 * units), BF16),
            pltpu.SemaphoreType.DMA((3, PIECES)),
        ],
        compiler_params=pltpu.CompilerParams(vmem_limit_bytes=56 * 2**20),
        cost_estimate=pl.CostEstimate(
            flops=4 * rows * width * units,
            bytes_accessed=2 * (rows * width + 2 * width * units + rows * units),
            transcendentals=rows * units,
        ),
    )(arrived, w_gate, w_up)


def down_kernel(hidden, own, fetched, left, right, low, high, out_ref):
    piece, side = fetched.shape[1], low.shape[1]
    here = lax.rem(lax.div(lax.axis_index("dp"), DP_STEP), SHARERS)
    groups, group = hidden.shape[0], lax.axis_index("etp")
    mine = hidden[group]
    others = jnp.concatenate(
        [hidden[lax.rem(group + groups - k, groups)] for k in range(1, groups)], axis=1
    )

    def project(start, block):
        columns = pl.ds(pl.multiple_of(start, side), block.shape[1])
        total = jnp.dot(mine, own[:, columns], preferred_element_type=F32)
        total += jnp.dot(others, block[...], preferred_element_type=F32)
        out_ref[:, columns] = total.astype(out_ref.dtype)

    project(here * piece, fetched)
    project(lax.rem(here + SHARERS - 1, SHARERS) * piece, left)
    project(lax.rem(here + 1, SHARERS) * piece, right)
    far = lax.rem(here + 2, SHARERS) * piece
    project(far, low)
    project(far + side, high)


def project_down(operands):
    groups, rows, units = operands[0].shape
    quarter = operands[1].shape[1]
    return pl.pallas_call(
        down_kernel,
        out_shape=jax.ShapeDtypeStruct((rows, quarter), BF16),
        in_specs=[IN_VMEM] * len(operands),
        out_specs=IN_VMEM,
        compiler_params=pltpu.CompilerParams(vmem_limit_bytes=16 * 2**20),
        cost_estimate=pl.CostEstimate(
            flops=2 * groups * rows * units * quarter,
            bytes_accessed=2 * groups * (rows * units + units * quarter) + 2 * rows * quarter,
            transcendentals=0,
        ),
    )(*operands)


def down_weights(w_down, quarter, quarters):
    here = lax.axis_index("etp")
    units, piece = w_down.shape[0], quarter // SHARERS
    block = (lax.axis_index("dp") // DP_STEP) % SHARERS
    own = lax.dynamic_slice(w_down, (0, here * quarter), (units, quarter))
    parts = [
        lax.dynamic_slice(w_down, (0, (here + k) % quarters * quarter + block * piece), (units, piece))
        for k in range(1, quarters)
    ]
    fetched = jnp.concatenate([shift(part, "etp", k) for k, part in enumerate(parts, 1)], axis=0)
    spread = (
        shift(fetched, "dp", DP_STEP),
        shift(fetched, "dp", -DP_STEP),
        shift(fetched[:, : piece // 2], "dp", 2 * DP_STEP),
        shift(fetched[:, piece // 2 :], "dp", -2 * DP_STEP),
    )
    return own, fetched, *spread


def per_device(tokens, expert_ids, route_weights, w_gate, w_up, w_down):
    tok_rows, width = tokens.shape
    route_count = expert_ids.shape[1]
    sources = lax.axis_size("expert")
    quarters = lax.axis_size("etp")
    experts = sources
    capacity = 2 * tok_rows * route_count // experts
    quarter = width // quarters

    outgoing, combine = dispatch_rows(expert_ids, route_weights, tokens, experts, capacity)
    arrived = lax.all_to_all(
        outgoing.reshape(experts, capacity, width), "expert", split_axis=0, concat_axis=0, tiled=True
    )
    blocks = down_weights(w_down[0], quarter, quarters)
    mine = hidden_units(arrived.reshape(sources * capacity, width), w_gate[0], w_up[0])
    gathered = lax.all_gather(mine, "etp")
    expert_out = project_down((gathered, *blocks))
    returned = lax.all_to_all(
        expert_out.reshape(sources, capacity, quarter), "expert", split_axis=0, concat_axis=0, tiled=True
    )
    return lax.dot_general(
        combine.reshape(experts * capacity, tok_rows),
        returned.reshape(experts * capacity, quarter),
        (((0,), (0,)), ((), ())),
        preferred_element_type=F32,
    ).astype(BF16)


def solution(mesh):
    return jax.shard_map(
        per_device,
        mesh=mesh,
        in_specs=(
            P(("dp", "expert"), None),
            P(("dp", "expert"), None),
            P(("dp", "expert"), None),
            P("expert", None, "etp"),
            P("expert", None, "etp"),
            P("expert", "etp", None),
        ),
        out_specs=P(("dp", "expert"), "etp"),
        check_vma=False,
    )
```

```python
import jax
import jax.numpy as jnp
from jax import lax
from jax.experimental import pallas as pl
from jax.experimental.pallas import tpu as pltpu
from jax.sharding import PartitionSpec as P


STEPS = 8
PIECES = (1, 3, 3, 3, 3, 3)
DP_STEP = 2
SHARERS = 4
BF16, F32 = jnp.bfloat16, jnp.float32
IN_VMEM = pl.BlockSpec(memory_space=pltpu.VMEM)
IN_HBM = pl.BlockSpec(memory_space=pltpu.HBM)


def shift(x, axis, by):
    count = lax.axis_size(axis)
    return lax.ppermute(x, axis, [(i, (i + by) % count) for i in range(count)])


def dispatch_kernel(
    ids_ref, weights_ref, tokens_ref, out_ref, combine_ref, ids, weights, tokens, out, combine, sems
):
    experts, capacity, rows = combine.shape
    routes, width = ids.shape[0], tokens.shape[1]
    reads = (
        pltpu.make_async_copy(ids_ref, ids, sems.at[0]),
        pltpu.make_async_copy(weights_ref, weights, sems.at[1]),
        pltpu.make_async_copy(tokens_ref, tokens, sems.at[2]),
    )
    for copy in reads:
        copy.start()
    expert = lax.broadcasted_iota(jnp.int32, (experts, rows), 0)
    place = lax.broadcasted_iota(jnp.int32, (experts, capacity, rows), 1)
    earlier = lax.broadcasted_iota(jnp.int32, (rows, rows), 0) < lax.broadcasted_iota(
        jnp.int32, (rows, rows), 1
    )
    reads[0].wait()
    named = jnp.zeros((experts, rows), F32)
    for k in range(routes):
        named = jnp.where(ids[k : k + 1, :] == expert, 1.0, named)
    slot = jnp.dot(
        named.astype(BF16), jnp.where(earlier, 1.0, 0.0).astype(BF16), preferred_element_type=F32
    ).astype(jnp.int32)
    slot = jnp.where(named > 0.0, slot, -1)
    taken = slot[:, None, :] == place
    chosen = jnp.where(taken, 1.0, 0.0).reshape(experts * capacity, rows).astype(BF16)
    reads[2].wait()
    writes = []
    for k in range(STEPS):
        cols = pl.ds(k * (width // STEPS), width // STEPS)
        out[:, cols] = jnp.dot(chosen, tokens[:, cols], preferred_element_type=F32).astype(BF16)
        writes.append(pltpu.make_async_copy(out.at[:, cols], out_ref.at[:, cols], sems.at[4 + k]))
        writes[-1].start()
    reads[1].wait()
    weight = jnp.zeros((experts, rows), F32)
    for k in range(routes):
        weight = jnp.where(ids[k : k + 1, :] == expert, weights[k : k + 1, :].astype(F32), weight)
    combine[...] = jnp.where(taken, weight[:, None, :], 0.0).astype(BF16)
    writes.append(pltpu.make_async_copy(combine, combine_ref, sems.at[3]))
    writes[-1].start()
    for copy in writes:
        copy.wait()


def dispatch_rows(expert_ids, route_weights, tokens, experts, capacity):
    rows, width = tokens.shape
    routes = expert_ids.shape[1]
    return pl.pallas_call(
        dispatch_kernel,
        out_shape=(
            jax.ShapeDtypeStruct((experts * capacity, width), BF16),
            jax.ShapeDtypeStruct((experts, capacity, rows), BF16),
        ),
        in_specs=[IN_HBM] * 3,
        out_specs=(IN_HBM, IN_HBM),
        scratch_shapes=[
            pltpu.VMEM((routes, rows), jnp.int32),
            pltpu.VMEM((routes, rows), BF16),
            pltpu.VMEM((rows, width), BF16),
            pltpu.VMEM((experts * capacity, width), BF16),
            pltpu.VMEM((experts, capacity, rows), BF16),
            pltpu.SemaphoreType.DMA((4 + STEPS,)),
        ],
        compiler_params=pltpu.CompilerParams(vmem_limit_bytes=60 * 2**20),
        cost_estimate=pl.CostEstimate(
            flops=2 * experts * capacity * rows * width,
            bytes_accessed=2 * (experts * capacity + rows) * width,
            transcendentals=0,
        ),
    )(expert_ids.T, route_weights.T, tokens)


def hidden_kernel(x_ref, gate_ref, up_ref, out_ref, x_buf, weights, sems):
    rows, width = x_ref.shape
    units = gate_ref.shape[1]
    depth = width // sum(PIECES)
    parts, copies = [], []
    for k, share in enumerate(PIECES):
        part = pl.ds(sum(PIECES[:k]) * depth, share * depth)
        parts.append(part)
        copies.append(
            (
                pltpu.make_async_copy(x_ref.at[:, part], x_buf.at[:, part], sems.at[2, k]),
                pltpu.make_async_copy(
                    gate_ref.at[part], weights.at[part, pl.ds(0, units)], sems.at[0, k]
                ),
                pltpu.make_async_copy(
                    up_ref.at[part], weights.at[part, pl.ds(units, units)], sems.at[1, k]
                ),
            )
        )
    for group in copies:
        for copy in group:
            copy.start()
    total = jnp.zeros((rows, 2 * units), F32)
    for k, part in enumerate(parts):
        for copy in copies[k]:
            copy.wait()
        total += jnp.dot(x_buf[:, part], weights[part, :], preferred_element_type=F32)
    gate, up = total[:, :units], total[:, units:]
    out_ref[...] = (gate / (1.0 + jnp.exp(-gate)) * up).astype(out_ref.dtype)


def hidden_units(arrived, w_gate, w_up):
    rows, width = arrived.shape
    units = w_gate.shape[1]
    return pl.pallas_call(
        hidden_kernel,
        out_shape=pltpu.VMEM((rows, units), BF16),
        in_specs=[IN_HBM] * 3,
        out_specs=IN_VMEM,
        scratch_shapes=[
            pltpu.VMEM((rows, width), BF16),
            pltpu.VMEM((width, 2 * units), BF16),
            pltpu.SemaphoreType.DMA((3, len(PIECES))),
        ],
        compiler_params=pltpu.CompilerParams(vmem_limit_bytes=56 * 2**20),
        cost_estimate=pl.CostEstimate(
            flops=4 * rows * width * units,
            bytes_accessed=2 * (rows * width + 2 * width * units + rows * units),
            transcendentals=rows * units,
        ),
    )(arrived, w_gate, w_up)


def down_kernel(hidden, own, fetched, left, right, low, high, out_ref):
    piece, side = fetched.shape[1], low.shape[1]
    here = lax.rem(lax.div(lax.axis_index("dp"), DP_STEP), SHARERS)
    groups, group = hidden.shape[0], lax.axis_index("etp")
    mine = hidden[group]
    others = jnp.concatenate(
        [hidden[lax.rem(group + groups - k, groups)] for k in range(1, groups)], axis=1
    )

    def project(start, block):
        columns = pl.ds(pl.multiple_of(start, side), block.shape[1])
        total = jnp.dot(mine, own[:, columns], preferred_element_type=F32)
        total += jnp.dot(others, block[...], preferred_element_type=F32)
        out_ref[:, columns] = total.astype(out_ref.dtype)

    project(here * piece, fetched)
    project(lax.rem(here + SHARERS - 1, SHARERS) * piece, left)
    project(lax.rem(here + 1, SHARERS) * piece, right)
    far = lax.rem(here + 2, SHARERS) * piece
    project(far, low)
    project(far + side, high)


def project_down(operands):
    groups, rows, units = operands[0].shape
    quarter = operands[1].shape[1]
    return pl.pallas_call(
        down_kernel,
        out_shape=jax.ShapeDtypeStruct((rows, quarter), BF16),
        in_specs=[IN_VMEM] * len(operands),
        out_specs=IN_VMEM,
        compiler_params=pltpu.CompilerParams(vmem_limit_bytes=16 * 2**20),
        cost_estimate=pl.CostEstimate(
            flops=2 * groups * rows * units * quarter,
            bytes_accessed=2 * groups * (rows * units + units * quarter) + 2 * rows * quarter,
            transcendentals=0,
        ),
    )(*operands)


def down_weights(w_down, quarter, quarters):
    here = lax.axis_index("etp")
    units, piece = w_down.shape[0], quarter // SHARERS
    block = (lax.axis_index("dp") // DP_STEP) % SHARERS
    own = lax.dynamic_slice(w_down, (0, here * quarter), (units, quarter))
    parts = [
        lax.dynamic_slice(w_down, (0, (here + k) % quarters * quarter + block * piece), (units, piece))
        for k in range(1, quarters)
    ]
    fetched = jnp.concatenate([shift(part, "etp", k) for k, part in enumerate(parts, 1)], axis=0)
    spread = (
        shift(fetched, "dp", DP_STEP),
        shift(fetched, "dp", -DP_STEP),
        shift(fetched[:, : piece // 2], "dp", 2 * DP_STEP),
        shift(fetched[:, piece // 2 :], "dp", -2 * DP_STEP),
    )
    return own, fetched, *spread


def per_device(tokens, expert_ids, route_weights, w_gate, w_up, w_down):
    tok_rows, width = tokens.shape
    route_count = expert_ids.shape[1]
    sources = lax.axis_size("expert")
    quarters = lax.axis_size("etp")
    experts = sources
    capacity = 2 * tok_rows * route_count // experts
    quarter = width // quarters

    outgoing, combine = dispatch_rows(expert_ids, route_weights, tokens, experts, capacity)
    arrived = lax.all_to_all(
        outgoing.reshape(experts, capacity, width), "expert", split_axis=0, concat_axis=0, tiled=True
    )
    blocks = down_weights(w_down[0], quarter, quarters)
    mine = hidden_units(arrived.reshape(sources * capacity, width), w_gate[0], w_up[0])
    gathered = lax.all_gather(mine, "etp")
    expert_out = project_down((gathered, *blocks))
    returned = lax.all_to_all(
        expert_out.reshape(sources, capacity, quarter), "expert", split_axis=0, concat_axis=0, tiled=True
    )
    return lax.dot_general(
        combine.reshape(experts * capacity, tok_rows),
        returned.reshape(experts * capacity, quarter),
        (((0,), (0,)), ((), ())),
        preferred_element_type=F32,
    ).astype(BF16)


def solution(mesh):
    return jax.shard_map(
        per_device,
        mesh=mesh,
        in_specs=(
            P(("dp", "expert"), None),
            P(("dp", "expert"), None),
            P(("dp", "expert"), None),
            P("expert", None, "etp"),
            P("expert", None, "etp"),
            P("expert", "etp", None),
        ),
        out_specs=P(("dp", "expert"), "etp"),
        check_vma=False,
    )
```
